32 devices in a mesh: dp: 2 (over core), layer: 2 (over x), col: 8 (over z, y).
Axes of the slice: x: 2, y: 2, z: 4, core: 2. Of those that a mesh axis runs over, the one named last changes fastest.
Arguments:
- tokens: bfloat16 [16, 256, 1024], P(None, 'dp', 'col'), parts along dimension 1, may hold values from -6 to 6
- w_input: bfloat16 [2, 1024, 4096], P('layer', None, 'col'), may hold values from -0.1875 to 0.1875
- w_recur: bfloat16 [2, 1024, 4096], P('layer', None, 'col'), may hold values from -0.1875 to 0.1875
- bias: float32 [2, 4096], P('layer', 'col'), may hold values from -1 to 5
Outputs:
- top_states: bfloat16 [16, 256, 1024], P('layer', 'dp', 'col'), parts along dimension 1
- final_h: bfloat16 [2, 256, 1024], P('layer', 'dp', 'col'), parts along dimension 1
- final_c: float32 [2, 256, 1024], P('layer', 'dp', 'col'), parts along dimension 1
The draws below stay inside these ranges and needn't reach their ends.
There are 2 independent parts, one for each index of `dp`. The reference program is written for one: setup_inputs(seed, part) draws one part's arguments, and reference() takes and returns one part's arrays. A program takes and returns all parts, laid end to end along the dimension named above; an argument that names none is the same for every part. Nothing has to cross between parts.
All inputs are finite; a program needn't handle non-finite values.
Results may differ from the reference program's by a relative error of at most 0.008.
Values may be sent and summed in bfloat16 or wider, within the bound.
A program may use at most 64 MiB of HBM per device.

```python
import jax
import jax.numpy as jnp
from jax import lax

H = 1024
GATES = 4096
SENT = 128
TSTEPS = 16
LAYERS = 2


def draw_bias(key, part):
    first, second, third, fourth = jax.random.split(jax.random.fold_in(key, 11), 4)
    others = jax.random.uniform(first, (LAYERS, H, 3), jnp.float32, -1.0, 1.0)
    strong = jax.random.uniform(second, (LAYERS, H), jnp.float32, 3.0, 5.0)
    weak = jax.random.uniform(third, (LAYERS, H), jnp.float32, -1.0, 1.0)
    keeper = jax.random.uniform(fourth, (LAYERS, H)) < 0.5
    forget = jnp.where(keeper, strong, weak)
    stacked = jnp.stack([others[:, :, 0], forget, others[:, :, 1], others[:, :, 2]], axis=-1)
    return stacked.reshape(LAYERS, 4 * H)


def level_of(key, dims, shards, smallest, high):
    factor_of, own = 1.0, jax.random.fold_in(key, 6)
    for position, shards_of in shards:
        steps = jnp.exp(jax.random.uniform(jax.random.fold_in(own, position), (shards_of,), jnp.float32, smallest / len(shards), high / len(shards)))
        factor_of = factor_of * jnp.repeat(steps, dims[position] // shards_of).reshape([-1 if axis == position else 1 for axis in range(len(dims))])
    return factor_of


def gaussian(key, extent, scale, most, cuts=(), dtype=jnp.bfloat16):
    array = jax.random.normal(key, extent, jnp.float32) * scale
    if len(cuts) > 0:
        array = level_of(key, extent, cuts, -0.22, 0.18) * array
    return jnp.clip(array, min=-most, max=most).astype(dtype)


def setup_inputs(seed: int = 0, part: int = 0) -> dict:
    streams_of = jax.random.split(jax.random.key(seed), 5)
    part_splits = jax.random.split(jax.random.fold_in(streams_of[4], part), 5)
    tokens = gaussian(part_splits[0], (TSTEPS, SENT, H), 1.0, 6.0, ((2, 8),))
    w_input = gaussian(streams_of[1], (LAYERS, H, GATES), H ** -0.5, 0.1875, ((0, 2), (2, 8)))
    w_recur = gaussian(streams_of[2], (LAYERS, H, GATES), H ** -0.5, 0.1875, ((0, 2), (2, 8)))
    bias = draw_bias(jax.random.fold_in(streams_of[4], 71), part)
    return {"tokens": tokens, "w_input": w_input, "w_recur": w_recur, "bias": bias}


def run_layer(layer_in, w_in, w_rec, gate_bias):
    sentences = layer_in.shape[1]
    width = w_rec.shape[0]

    def advance(carry, x_step):
        hidden, cell = carry
        gates = jnp.dot(x_step, w_in, preferred_element_type=jnp.float32)
        gates = gates + jnp.dot(hidden, w_rec, preferred_element_type=jnp.float32) + gate_bias
        gates = gates.reshape(sentences, width, 4)
        in_gate = jax.nn.sigmoid(gates[:, :, 0])
        forget = jax.nn.sigmoid(gates[:, :, 1])
        update = jnp.tanh(gates[:, :, 2])
        out_gate = jax.nn.sigmoid(gates[:, :, 3])
        cell = forget * cell + in_gate * update
        hidden = (out_gate * jnp.tanh(cell)).astype(jnp.bfloat16)
        return (hidden, cell), hidden

    start = (jnp.zeros((sentences, width), jnp.bfloat16), jnp.zeros((sentences, width), jnp.float32))
    (hidden, cell), states = lax.scan(advance, start, layer_in)
    return hidden, cell, states


def reference(tokens, w_input, w_recur, bias):
    layer_in = tokens
    last_h = []
    last_c = []
    states = tokens
    for level in range(LAYERS):
        hidden, cell, states = run_layer(layer_in, w_input[level], w_recur[level], bias[level])
        last_h.append(hidden)
        last_c.append(cell)
        if level >= 1:
            layer_in = (states.astype(jnp.float32) + layer_in.astype(jnp.float32)).astype(jnp.bfloat16)
        else:
            layer_in = states
    return states, jnp.stack(last_h), jnp.stack(last_c)
```

```python
import functools

import jax
import jax.numpy as jnp
from jax import lax
from jax.experimental import pallas as pl
from jax.experimental.pallas import tpu as pltpu
from jax.sharding import PartitionSpec as P


def passed_along(block, axis, distance):
    devices = range(lax.axis_size(axis))
    route = [(i - distance, i) for i in devices if i - distance in devices]
    return lax.ppermute(block, axis, route)


def broadcast(block, axis, source):
    block = jnp.where(lax.axis_index(axis) == source, block, jnp.zeros_like(block))
    return lax.psum(block, axis)


def shards(tokens, w_input, w_recur, bias):
    steps_count, sentences, units = tokens.shape
    w_local = w_input[0]
    r_local = w_recur[0]
    b_local = bias[0]
    layers = lax.axis_size("layer")
    level = lax.axis_index("layer")
    is_first = level == 0
    has_skip = level >= 1
    is_last = level == layers - 1

    def cell_step(gates, cell):
        gates = gates.reshape(sentences, units, 4)
        in_gate = jax.nn.sigmoid(gates[:, :, 0])
        forget = jax.nn.sigmoid(gates[:, :, 1])
        update = jnp.tanh(gates[:, :, 2])
        out_gate = jax.nn.sigmoid(gates[:, :, 3])
        cell_new = forget * cell + in_gate * update
        hidden_new = (out_gate * jnp.tanh(cell_new)).astype(jnp.bfloat16)
        return (hidden_new, cell_new)

    def skip_sum(hidden_new, in_part):
        summed = (hidden_new.astype(jnp.float32) + in_part.astype(jnp.float32)).astype(jnp.bfloat16)
        return jnp.where(has_skip, summed, hidden_new)

    zero_h = jnp.zeros((sentences, units), jnp.bfloat16)
    zero_c = jnp.zeros((sentences, units), jnp.float32)
    buffer = jnp.zeros((steps_count, sentences, units), jnp.bfloat16)
    span = 4
    count = steps_count // span
    block_sections = count + layers - 1
    zero_span = jnp.zeros((span, sentences, units), jnp.bfloat16)

    def section_block(section, carry):
        hidden, cell, outgoing, kept = carry
        which = section - level
        active = (which >= 0) & (which < count)
        first_step = jnp.clip(which, 0, count - 1) * span
        own_tokens = lax.dynamic_slice_in_dim(tokens, first_step, span, 0)
        received = passed_along(outgoing, "layer", 1)
        in_part = jnp.where(is_first, own_tokens, received)
        in_full = lax.all_gather(in_part, "col", axis=2, tiled=True)
        projected = jnp.dot(
            in_full.reshape(span * sentences, in_full.shape[2]),
            w_local,
            preferred_element_type=jnp.float32,
        )
        projected = projected.reshape(span, sentences, w_local.shape[1])
        states = []
        for offset in range(span):
            h_full = lax.all_gather(hidden, "col", axis=1, tiled=True)
            gates = (
                projected[offset]
                + jnp.dot(h_full, r_local, preferred_element_type=jnp.float32)
                + b_local
            )
            hidden_new, cell_new = cell_step(gates, cell)
            hidden = jnp.where(active, hidden_new, hidden)
            cell = jnp.where(active, cell_new, cell)
            states.append(hidden_new)
        produced = jnp.stack(states)
        outgoing = skip_sum(produced, in_part)
        written = lax.dynamic_update_slice_in_dim(kept, produced, first_step, 0)
        kept = jnp.where(active & is_last, written, kept)
        return (hidden, cell, outgoing, kept)

    hidden, cell, outgoing, buffer = lax.fori_loop(
        0, block_sections, section_block, (zero_h, zero_c, zero_span, buffer)
    )
    everything = broadcast(buffer, "layer", layers - 1)
    block = steps_count // layers
    top_states = lax.dynamic_slice_in_dim(everything, level * block, block, 0)
    return (top_states, hidden[None], cell[None])


MESH = pl.DeviceIdType.MESH
CHUNK = 4


def lstm_kernel(
    groups,
    tokens, w_in, w_rec, bias,
    top, final_h, final_c,
    xs, hs, wi, wr, raw_in, raw_rec, braw, bperm, cell, gates,
    send_sem, x_sem, h_sem, tok_y_sem, tok_z_sem, w_y_sem, w_d_sem, b_sem, top_sem, fin_sem,
):
    steps, sentences, units = tokens.shape
    half = sentences // 2
    depth = w_in.shape[0]
    part_rows = depth // 2
    chunks = steps // CHUNK
    keep = steps // 2
    dp = lax.axis_index("dp")
    level = lax.axis_index("layer")
    col = lax.axis_index("col")
    p = col // 2
    q = lax.rem(col, 2)
    other = 1 - q
    pair = {"col": 2 * p + other}
    twin = {"dp": 1 - dp}
    is_first = level == 0
    is_last = level == 1

    def copy(src, dst, sem, device):
        return pltpu.make_async_remote_copy(
            src_ref=src, dst_ref=dst, send_sem=send_sem, recv_sem=sem,
            device_id=device, device_id_type=MESH,
        )

    def near(i):
        return lax.rem(p + i, groups)

    barrier = pltpu.get_barrier_semaphore()
    targets = [{"col": 2 * near(i) + q} for i in range(1, groups)]
    targets += [pair, twin]
    targets += [{"layer": 1 - level, "col": 2 * near(i) + q} for i in range(groups)]
    targets += [{"layer": 1 - level, "col": 2 * p + other}]
    for device in targets:
        pl.semaphore_signal(barrier, inc=1, device_id=device, device_id_type=MESH)
    pl.semaphore_wait(barrier, len(targets))

    my_rows = pl.ds(pl.multiple_of(q * half, half), half)
    other_rows = pl.ds(pl.multiple_of(other * half, half), half)

    def span(c):
        return pl.ds(c * CHUNK, CHUNK)

    def tok_to_pair(c):
        return copy(tokens.at[span(c), other_rows], xs.at[span(c), p, q], tok_y_sem.at[c], pair)

    def tok_from_pair(c):
        place = xs.at[span(c), p, other]
        return copy(place, place, tok_y_sem.at[c], pair)

    def tok_own(c, i):
        return copy(tokens.at[span(c), my_rows], xs.at[span(c), p, q], tok_z_sem.at[c, p, q], {"col": 2 * near(i) + q})

    def tok_forward(c, i):
        place = xs.at[span(c), p, other]
        return copy(place, place, tok_z_sem.at[c, p, other], {"col": 2 * near(i) + q})

    def tok_arrived(c, i, y):
        place = xs.at[span(c), near(i), y]
        return copy(place, place, tok_z_sem.at[c, near(i), y], pair)

    part = pl.ds(pl.multiple_of(dp * part_rows, part_rows), part_rows)
    twin_part = pl.ds(pl.multiple_of((1 - dp) * part_rows, part_rows), part_rows)
    weights = ((w_in, raw_in), (w_rec, raw_rec))

    def w_to_pair(k):
        own, raw = weights[k]
        return copy(own.at[part], raw.at[part], w_y_sem.at[k], pair)

    def w_to_twin(k):
        raw = weights[k][1]
        return copy(raw.at[part], raw.at[part], w_d_sem.at[k], twin)

    def w_from_twin(k):
        raw = weights[k][1]
        return copy(raw.at[twin_part], raw.at[twin_part], w_d_sem.at[k], twin)

    bias_copy = copy(bias, braw, b_sem, pair)

    @pl.when(is_first)
    def _():
        tok_to_pair(0).start()
        for i in range(1, groups):
            tok_own(0, i).start()

    bias_copy.start()
    w_to_pair(0).start()
    w_to_pair(1).start()

    @pl.when(is_first)
    def _():
        for c in range(1, chunks):
            tok_to_pair(c).start()
        for t in range(steps):
            xs[t, p, q] = tokens[t, my_rows]

    cell[...] = jnp.zeros_like(cell)
    width = 4 * units
    row = lax.broadcasted_iota(jnp.int32, (width, width), 0)
    column = lax.broadcasted_iota(jnp.int32, (width, width), 1)
    spread = row == 4 * lax.rem(column, units) + column // units
    order = jnp.where(spread, 1.0, 0.0).astype(jnp.bfloat16)
    block_rows = 256

    def regroup(src, dst, which):
        @pl.loop(0, depth // block_rows)
        def _(r):
            rows = pl.ds(pl.multiple_of(r * block_rows, block_rows), block_rows)
            moved = jnp.dot(src[rows], order, preferred_element_type=jnp.float32)
            dst[which, rows] = moved.astype(jnp.bfloat16)

    def regroup_bias(src, which):
        value = jnp.broadcast_to(src[...], (8, width))
        total = jnp.zeros((8, width), jnp.float32)
        for _ in range(3):
            piece = value.astype(jnp.bfloat16)
            total = total + jnp.dot(piece, order, preferred_element_type=jnp.float32)
            value = value - piece.astype(jnp.float32)
        bperm[which] = total

    regroup(w_in, wi, q)
    regroup_bias(bias, q)

    @pl.when(is_first)
    def _():
        tok_from_pair(0).wait_recv()
        for i in range(1, groups):
            tok_forward(0, i).start()

    regroup(w_rec, wr, q)
    bias_copy.wait_recv()
    regroup_bias(braw, other)
    w_to_pair(0).wait_recv()
    w_to_twin(0).start()
    w_from_twin(0).wait_recv()
    regroup(raw_in, wi, other)

    def to_peer(t, i):
        return copy(hs.at[t, p], hs.at[t, p], h_sem.at[t, p], {"col": 2 * near(i) + q})

    def from_peer(t, i):
        return copy(hs.at[t, near(i)], hs.at[t, near(i)], h_sem.at[t, near(i)], pair)

    def to_next(t, i):
        return copy(hs.at[t, p], xs.at[t, p], x_sem.at[t, p], {"layer": 1 - level, "col": 2 * near(i) + q})

    def from_before(t, i):
        return copy(xs.at[t, near(i)], xs.at[t, near(i)], x_sem.at[t, near(i)], pair)

    def joined(ref, t):
        return jnp.concatenate([ref[t, g, y] for g in range(groups) for y in range(2)], axis=1)

    def top_far(t, b):
        return copy(hs.at[t, p, b], top.at[t, my_rows], top_sem.at[t, q], {"layer": 1 - level, "col": 2 * p + b})

    def top_pair(t):
        return copy(hs.at[t, p, other], top.at[t - keep, my_rows], top_sem.at[t - keep, q], pair)

    @pl.loop(0, steps)
    def _(t):
        @pl.when(is_first & (lax.rem(t, CHUNK) == 0))
        def _():
            c = t // CHUNK
            for i in range(1, groups):
                tok_arrived(c, i, 0).wait_recv()
                tok_arrived(c, i, 1).wait_recv()

        @pl.when(is_last)
        def _():
            for i in range(groups):
                from_before(t, i).wait_recv()

        given = joined(xs, t)
        for b in range(2):
            gates[b] = jnp.dot(given, wi[b], preferred_element_type=jnp.float32) + bperm[b, 0:1]

        @pl.when(t == 1)
        def _():
            w_to_pair(1).wait_recv()
            w_to_twin(1).start()
            w_from_twin(1).wait_recv()
            regroup(raw_rec, wr, other)

        @pl.when(t > 0)
        def _():
            for i in range(1, groups):
                from_peer(t - 1, i).wait_recv()
            state = joined(hs, t - 1)
            for b in range(2):
                gates[b] += jnp.dot(state, wr[b], preferred_element_type=jnp.float32)

        for b in range(2):
            in_gate = 0.5 * jnp.tanh(0.5 * gates[b, :, 0:units]) + 0.5
            forget = 0.5 * jnp.tanh(0.5 * gates[b, :, units : 2 * units]) + 0.5
            update = jnp.tanh(gates[b, :, 2 * units : 3 * units])
            out_gate = 0.5 * jnp.tanh(0.5 * gates[b, :, 3 * units :]) + 0.5
            cell_new = forget * cell[b] + in_gate * update
            cell[b] = cell_new
            hs[t, p, b] = (out_gate * jnp.tanh(cell_new)).astype(jnp.bfloat16)

        @pl.when(t < steps - 1)
        def _():
            for i in range(1, groups):
                to_peer(t, i).start()

        @pl.when(is_first)
        def _():
            for i in range(groups):
                to_next(t, i).start()

            @pl.when((lax.rem(t, CHUNK) == 1) & (t < steps - CHUNK))
            def _():
                c = t // CHUNK + 1
                tok_from_pair(c).wait_recv()
                for i in range(1, groups):
                    tok_own(c, i).start()
                    tok_forward(c, i).start()

        @pl.when(is_last & (t < keep))
        def _():
            top_far(t, 0).start()
            top_far(t, 1).start()

        @pl.when(is_last & (t >= keep))
        def _():
            top_pair(t).start()
            top[t - keep, my_rows] = hs[t, p, q]

    end = steps - 1
    fin_h = copy(hs.at[end, p, other], final_h.at[0, my_rows], fin_sem.at[0], pair)
    fin_c = copy(cell.at[other], final_c.at[0, my_rows], fin_sem.at[1], pair)
    fin_h.start()
    fin_c.start()
    final_h[0, my_rows] = hs[end, p, q]
    final_c[0, my_rows] = cell[q]

    bias_copy.wait_send()
    for k in range(2):
        w_to_pair(k).wait_send()
        w_to_twin(k).wait_send()
    fin_h.wait()
    fin_c.wait()

    @pl.loop(0, end)
    def _(t):
        for i in range(1, groups):
            to_peer(t, i).wait_send()

    @pl.when(is_first)
    def _():
        for c in range(chunks):
            tok_to_pair(c).wait_send()
            for i in range(1, groups):
                tok_own(c, i).wait_send()
                tok_forward(c, i).wait_send()

        @pl.loop(0, steps)
        def _(t):
            for i in range(groups):
                to_next(t, i).wait_send()

        @pl.loop(0, keep)
        def _(t):
            for y in range(2):
                rows = top.at[t, pl.ds(y * half, half)]
                copy(rows, rows, top_sem.at[t, y], pair).wait_recv()

    @pl.when(is_last)
    def _():
        @pl.loop(0, keep)
        def _(t):
            top_far(t, 0).wait_send()
            top_far(t, 1).wait_send()
            top_pair(t + keep).wait_send()
            rows = top.at[t, other_rows]
            copy(rows, rows, top_sem.at[t, other], pair).wait_recv()


def fused(tokens, w_input, w_recur, bias):
    steps, sentences, units = tokens.shape
    depth, width = w_input.shape[1:]
    groups = lax.axis_size("col") // 2
    half = sentences // 2
    bf16, f32, dma = jnp.bfloat16, jnp.float32, pltpu.SemaphoreType.DMA
    vmem = pl.BlockSpec(memory_space=pltpu.VMEM)
    return pl.pallas_call(
        functools.partial(lstm_kernel, groups),
        out_shape=(
            jax.ShapeDtypeStruct((steps // 2, sentences, units), bf16),
            jax.ShapeDtypeStruct((1, sentences, units), bf16),
            jax.ShapeDtypeStruct((1, sentences, units), f32),
        ),
        in_specs=[vmem] * 4,
        out_specs=(vmem, vmem, vmem),
        scratch_shapes=[
            pltpu.VMEM((steps, groups, 2, half, units), bf16),
            pltpu.VMEM((steps, groups, 2, half, units), bf16),
            pltpu.VMEM((2, depth, width), bf16),
            pltpu.VMEM((2, depth, width), bf16),
            pltpu.VMEM((depth, width), bf16),
            pltpu.VMEM((depth, width), bf16),
            pltpu.VMEM((1, width), f32),
            pltpu.VMEM((2, 8, width), f32),
            pltpu.VMEM((2, half, units), f32),
            pltpu.VMEM((2, half, width), f32),
            dma,
            dma((steps, groups)),
            dma((steps, groups)),
            dma((steps // CHUNK,)),
            dma((steps // CHUNK, groups, 2)),
            dma((2,)),
            dma((2,)),
            dma,
            dma((steps // 2, 2)),
            dma((2,)),
        ],
        compiler_params=pltpu.CompilerParams(
            collective_id=0, has_side_effects=True, vmem_limit_bytes=48 * 2**20
        ),
        name="lstm",
    )(tokens, w_input[0], w_recur[0], bias)


def solution(mesh):
    in_specs = (
        P(None, "dp", "col"),
        P("layer", None, "col"),
        P("layer", None, "col"),
        P("layer", "col"),
    )
    out_specs = (P("layer", "dp", "col"), P("layer", "dp", "col"), P("layer", "dp", "col"))
    cols = mesh.shape["col"]

    def body(tokens, w_input, w_recur, bias):
        steps, sentences, units = tokens.shape
        fits = mesh.shape["layer"] == 2 and mesh.shape["dp"] == 2 and cols % 2 == 0
        fits = fits and units % 128 == 0 and sentences % 32 == 0 and steps % CHUNK == 0
        return (fused if fits else shards)(tokens, w_input, w_recur, bias)

    return jax.shard_map(body, mesh=mesh, in_specs=in_specs, out_specs=out_specs, check_vma=False)
```

```python
import functools

import jax
import jax.numpy as jnp
from jax import lax
from jax.experimental import pallas as pl
from jax.experimental.pallas import tpu as pltpu
from jax.sharding import PartitionSpec as P


def passed_along(block, axis, distance):
    devices = range(lax.axis_size(axis))
    route = [(i - distance, i) for i in devices if i - distance in devices]
    return lax.ppermute(block, axis, route)


def broadcast(block, axis, source):
    block = jnp.where(lax.axis_index(axis) == source, block, jnp.zeros_like(block))
    return lax.psum(block, axis)


def shards(tokens, w_input, w_recur, bias):
    steps_count, sentences, units = tokens.shape
    w_local = w_input[0]
    r_local = w_recur[0]
    b_local = bias[0]
    layers = lax.axis_size("layer")
    level = lax.axis_index("layer")
    is_first = level == 0
    has_skip = level >= 1
    is_last = level == layers - 1

    def cell_step(gates, cell):
        gates = gates.reshape(sentences, units, 4)
        in_gate = jax.nn.sigmoid(gates[:, :, 0])
        forget = jax.nn.sigmoid(gates[:, :, 1])
        update = jnp.tanh(gates[:, :, 2])
        out_gate = jax.nn.sigmoid(gates[:, :, 3])
        cell_new = forget * cell + in_gate * update
        hidden_new = (out_gate * jnp.tanh(cell_new)).astype(jnp.bfloat16)
        return (hidden_new, cell_new)

    def skip_sum(hidden_new, in_part):
        summed = (hidden_new.astype(jnp.float32) + in_part.astype(jnp.float32)).astype(jnp.bfloat16)
        return jnp.where(has_skip, summed, hidden_new)

    zero_h = jnp.zeros((sentences, units), jnp.bfloat16)
    zero_c = jnp.zeros((sentences, units), jnp.float32)
    buffer = jnp.zeros((steps_count, sentences, units), jnp.bfloat16)
    span = 4
    count = steps_count // span
    block_sections = count + layers - 1
    zero_span = jnp.zeros((span, sentences, units), jnp.bfloat16)

    def section_block(section, carry):
        hidden, cell, outgoing, kept = carry
        which = section - level
        active = (which >= 0) & (which < count)
        first_step = jnp.clip(which, 0, count - 1) * span
        own_tokens = lax.dynamic_slice_in_dim(tokens, first_step, span, 0)
        received = passed_along(outgoing, "layer", 1)
        in_part = jnp.where(is_first, own_tokens, received)
        in_full = lax.all_gather(in_part, "col", axis=2, tiled=True)
        projected = jnp.dot(
            in_full.reshape(span * sentences, in_full.shape[2]),
            w_local,
            preferred_element_type=jnp.float32,
        )
        projected = projected.reshape(span, sentences, w_local.shape[1])
        states = []
        for offset in range(span):
            h_full = lax.all_gather(hidden, "col", axis=1, tiled=True)
            gates = (
                projected[offset]
                + jnp.dot(h_full, r_local, preferred_element_type=jnp.float32)
                + b_local
            )
            hidden_new, cell_new = cell_step(gates, cell)
            hidden = jnp.where(active, hidden_new, hidden)
            cell = jnp.where(active, cell_new, cell)
            states.append(hidden_new)
        produced = jnp.stack(states)
        outgoing = skip_sum(produced, in_part)
        written = lax.dynamic_update_slice_in_dim(kept, produced, first_step, 0)
        kept = jnp.where(active & is_last, written, kept)
        return (hidden, cell, outgoing, kept)

    hidden, cell, outgoing, buffer = lax.fori_loop(
        0, block_sections, section_block, (zero_h, zero_c, zero_span, buffer)
    )
    everything = broadcast(buffer, "layer", layers - 1)
    block = steps_count // layers
    top_states = lax.dynamic_slice_in_dim(everything, level * block, block, 0)
    return (top_states, hidden[None], cell[None])


MESH = pl.DeviceIdType.MESH
CHUNK = 4


def lstm_kernel(
    groups,
    tokens, w_in, w_rec, bias,
    top, final_h, final_c,
    xs, hs, ts, wi, wr, own_in, own_rec, raw_in, raw_rec, braw, bperm, cell, gates,
    send_sem, x_sem, h_sem, tok_y_sem, tok_z_sem, tok_x_sem, tok_own_sem,
    w_own_sem, w_y_sem, w_d_sem, b_sem, top_sem, fin_sem,
):
    steps, sentences, units = tokens.shape
    half = sentences // 2
    depth = w_in.shape[0]
    part_rows = depth // 2
    keep = steps // 2
    chunks = keep // CHUNK
    dp = lax.axis_index("dp")
    level = lax.axis_index("layer")
    col = lax.axis_index("col")
    p = col // 2
    q = lax.rem(col, 2)
    other = 1 - q
    pair = {"col": 2 * p + other}
    twin = {"dp": 1 - dp}
    is_first = level == 0
    is_last = level == 1

    def copy(src, dst, sem, device):
        return pltpu.make_async_remote_copy(
            src_ref=src, dst_ref=dst, send_sem=send_sem, recv_sem=sem,
            device_id=device, device_id_type=MESH,
        )

    def near(i):
        return lax.rem(p + i, groups)

    barrier = pltpu.get_barrier_semaphore()
    targets = [{"col": 2 * near(i) + q} for i in range(1, groups)]
    targets += [pair, twin]
    targets += [{"layer": 1 - level, "col": 2 * p + y} for y in range(2)]
    for device in targets:
        pl.semaphore_signal(barrier, inc=1, device_id=device, device_id_type=MESH)
    pl.semaphore_wait(barrier, len(targets))

    my_rows = pl.ds(pl.multiple_of(q * half, half), half)
    other_rows = pl.ds(pl.multiple_of(other * half, half), half)

    def span(c):
        return pl.ds(c * CHUNK, CHUNK)

    def source(c):
        return pl.ds(level * keep + c * CHUNK, CHUNK)

    def tok_local(buf, c):
        return pltpu.make_async_copy(tokens.at[source(c), my_rows], buf.at[span(c), p, q], tok_own_sem.at[c])

    def tok_to_pair(buf, c):
        return copy(tokens.at[source(c), other_rows], buf.at[span(c), p, q], tok_y_sem.at[c], pair)

    def tok_from_pair(buf, c):
        place = buf.at[span(c), p, other]
        return copy(place, place, tok_y_sem.at[c], pair)

    def tok_own(buf, c, i):
        return copy(tokens.at[source(c), my_rows], buf.at[span(c), p, q], tok_z_sem.at[c, p, q], {"col": 2 * near(i) + q})

    def tok_forward(buf, c, i):
        place = buf.at[span(c), p, other]
        return copy(place, place, tok_z_sem.at[c, p, other], {"col": 2 * near(i) + q})

    def tok_arrived(buf, c, i, y):
        place = buf.at[span(c), near(i), y]
        return copy(place, place, tok_z_sem.at[c, near(i), y], pair)

    def tok_over(c):
        return copy(ts.at[span(c)], xs.at[pl.ds(keep + c * CHUNK, CHUNK)], tok_x_sem.at[c], {"layer": 1 - level})

    def tok_all(buf, c):
        for i in range(1, groups):
            tok_arrived(buf, c, i, 0).wait_recv()
            tok_arrived(buf, c, i, 1).wait_recv()

    part = pl.ds(pl.multiple_of(dp * part_rows, part_rows), part_rows)
    twin_part = pl.ds(pl.multiple_of((1 - dp) * part_rows, part_rows), part_rows)
    weights = ((w_in, raw_in), (w_rec, raw_rec))

    def w_to_pair(k):
        own, raw = weights[k]
        return copy(own.at[part], raw.at[part], w_y_sem.at[k], pair)

    def w_to_twin(k):
        raw = weights[k][1]
        return copy(raw.at[part], raw.at[part], w_d_sem.at[k], twin)

    def w_from_twin(k):
        raw = weights[k][1]
        return copy(raw.at[twin_part], raw.at[twin_part], w_d_sem.at[k], twin)

    bias_copy = copy(bias, braw, b_sem, pair)

    def own_weights(k):
        return pltpu.make_async_copy(weights[k][0], (own_in, own_rec)[k], w_own_sem.at[k])

    @pl.when(is_first)
    def _():
        tok_to_pair(xs, 0).start()
        for i in range(1, groups):
            tok_own(xs, 0, i).start()

    @pl.when(is_last)
    def _():
        for c in range(chunks):
            tok_to_pair(ts, c).start()
        for i in range(1, groups):
            tok_own(ts, 0, i).start()

    own_weights(0).start()
    bias_copy.start()
    w_to_pair(0).start()

    @pl.when(is_first)
    def _():
        for c in range(1, chunks):
            tok_to_pair(xs, c).start()
        for c in range(chunks):
            tok_local(xs, c).start()

    @pl.when(is_last)
    def _():
        for c in range(chunks):
            tok_local(ts, c).start()

    own_weights(1).start()
    w_to_pair(1).start()

    cell[...] = jnp.zeros_like(cell)
    width = 4 * units
    row = lax.broadcasted_iota(jnp.int32, (width, width), 0)
    column = lax.broadcasted_iota(jnp.int32, (width, width), 1)
    spread = row == 4 * lax.rem(column, units) + column // units
    order = jnp.where(spread, 1.0, 0.0).astype(jnp.bfloat16)
    block_rows = 256

    def regroup(src, dst, which):
        @pl.loop(0, depth // block_rows)
        def _(r):
            rows = pl.ds(pl.multiple_of(r * block_rows, block_rows), block_rows)
            moved = jnp.dot(src[rows], order, preferred_element_type=jnp.float32)
            dst[which, rows] = moved.astype(jnp.bfloat16)

    def regroup_bias(src, which):
        value = jnp.broadcast_to(src[...], (8, width))
        total = jnp.zeros((8, width), jnp.float32)
        for _ in range(3):
            piece = value.astype(jnp.bfloat16)
            total = total + jnp.dot(piece, order, preferred_element_type=jnp.float32)
            value = value - piece.astype(jnp.float32)
        bperm[which] = total

    own_weights(0).wait()
    regroup(own_in, wi, q)
    regroup_bias(bias, q)

    def hand_on(buf):
        for c in range(chunks):
            tok_from_pair(buf, c).wait_recv()
            for i in range(1, groups):
                tok_forward(buf, c, i).start()
            if c + 1 < chunks:
                for i in range(1, groups):
                    tok_own(buf, c + 1, i).start()

    @pl.when(is_last)
    def _():
        hand_on(ts)

    @pl.when(is_first)
    def _():
        tok_from_pair(xs, 0).wait_recv()
        for i in range(1, groups):
            tok_forward(xs, 0, i).start()
        for c in range(1, chunks):
            for i in range(1, groups):
                tok_own(xs, c, i).start()

    own_weights(1).wait()
    regroup(own_rec, wr, q)
    bias_copy.wait_recv()
    regroup_bias(braw, other)
    w_to_pair(0).wait_recv()
    w_to_twin(0).start()
    w_from_twin(0).wait_recv()
    regroup(raw_in, wi, other)

    @pl.when(is_first)
    def _():
        for c in range(1, chunks):
            tok_from_pair(xs, c).wait_recv()
            for i in range(1, groups):
                tok_forward(xs, c, i).start()

    @pl.when(is_last)
    def _():
        for c in range(chunks):
            tok_local(ts, c).wait()
            tok_all(ts, c)
            tok_over(c).start()

    def to_peer(t, i):
        return copy(hs.at[t, p], hs.at[t, p], h_sem.at[t, p], {"col": 2 * near(i) + q})

    def from_peer(t, i):
        return copy(hs.at[t, near(i)], hs.at[t, near(i)], h_sem.at[t, near(i)], pair)

    def to_next(t, g):
        return copy(hs.at[t, g], xs.at[t, g], x_sem.at[t, g], {"layer": 1 - level})

    def joined(ref, t):
        return jnp.concatenate([ref[t, g, y] for g in range(groups) for y in range(2)], axis=1)

    def top_far(t, b):
        return copy(hs.at[t, p, b], top.at[t, my_rows], top_sem.at[t, q], {"layer": 1 - level, "col": 2 * p + b})

    def top_pair(t):
        return copy(hs.at[t, p, other], top.at[t - keep, my_rows], top_sem.at[t - keep, q], pair)

    def peers_in(t):
        for i in range(1, groups):
            from_peer(t, i).wait_recv()

            @pl.when(is_first)
            def _():
                to_next(t, near(i)).start()

    @pl.loop(0, steps)
    def _(t):
        @pl.when(is_first & (lax.rem(t, CHUNK) == 0))
        def _():
            c = lax.rem(t // CHUNK, chunks)

            @pl.when(t < keep)
            def _():
                tok_local(xs, c).wait()
                tok_all(xs, c)

            @pl.when(t >= keep)
            def _():
                tok_over(c).wait_recv()

        @pl.when(is_last)
        def _():
            for g in range(groups):
                to_next(t, g).wait_recv()

        given = joined(xs, t)
        for b in range(2):
            gates[b] = jnp.dot(given, wi[b], preferred_element_type=jnp.float32) + bperm[b, 0:1]

        @pl.when(t == 1)
        def _():
            w_to_pair(1).wait_recv()
            w_to_twin(1).start()
            w_from_twin(1).wait_recv()
            regroup(raw_rec, wr, other)

        @pl.when(t > 0)
        def _():
            peers_in(t - 1)
            state = joined(hs, t - 1)
            for b in range(2):
                gates[b] += jnp.dot(state, wr[b], preferred_element_type=jnp.float32)

        for b in range(2):
            in_gate = 0.5 * jnp.tanh(0.5 * gates[b, :, 0:units]) + 0.5
            forget = 0.5 * jnp.tanh(0.5 * gates[b, :, units : 2 * units]) + 0.5
            update = jnp.tanh(gates[b, :, 2 * units : 3 * units])
            out_gate = 0.5 * jnp.tanh(0.5 * gates[b, :, 3 * units :]) + 0.5
            cell_new = forget * cell[b] + in_gate * update
            cell[b] = cell_new
            hs[t, p, b] = (out_gate * jnp.tanh(cell_new)).astype(jnp.bfloat16)

        @pl.when(is_first | (t < steps - 1))
        def _():
            for i in range(1, groups):
                to_peer(t, i).start()

        @pl.when(is_first)
        def _():
            to_next(t, p).start()

        @pl.when(is_last & (t < keep))
        def _():
            top_far(t, 0).start()
            top_far(t, 1).start()

        @pl.when(is_last & (t >= keep))
        def _():
            top_pair(t).start()
            top[t - keep, my_rows] = hs[t, p, q]

    end = steps - 1

    @pl.when(is_first)
    def _():
        peers_in(end)

    fin_h = copy(hs.at[end, p, other], final_h.at[0, my_rows], fin_sem.at[0], pair)
    fin_c = copy(cell.at[other], final_c.at[0, my_rows], fin_sem.at[1], pair)
    fin_h.start()
    fin_c.start()
    final_h[0, my_rows] = hs[end, p, q]
    final_c[0, my_rows] = cell[q]

    bias_copy.wait_send()
    for k in range(2):
        w_to_pair(k).wait_send()
        w_to_twin(k).wait_send()
    fin_h.wait()
    fin_c.wait()

    @pl.loop(0, end)
    def _(t):
        for i in range(1, groups):
            to_peer(t, i).wait_send()

    def tokens_sent(buf):
        for c in range(chunks):
            tok_to_pair(buf, c).wait_send()
            for i in range(1, groups):
                tok_own(buf, c, i).wait_send()
                tok_forward(buf, c, i).wait_send()

    @pl.when(is_first)
    def _():
        tokens_sent(xs)
        for i in range(1, groups):
            to_peer(end, i).wait_send()

        @pl.loop(0, steps)
        def _(t):
            for g in range(groups):
                to_next(t, g).wait_send()

        @pl.loop(0, keep)
        def _(t):
            for y in range(2):
                rows = top.at[t, pl.ds(y * half, half)]
                copy(rows, rows, top_sem.at[t, y], pair).wait_recv()

    @pl.when(is_last)
    def _():
        tokens_sent(ts)
        for c in range(chunks):
            tok_over(c).wait_send()

        @pl.loop(0, keep)
        def _(t):
            top_far(t, 0).wait_send()
            top_far(t, 1).wait_send()
            top_pair(t + keep).wait_send()
            rows = top.at[t, other_rows]
            copy(rows, rows, top_sem.at[t, other], pair).wait_recv()


def fused(tokens, w_input, w_recur, bias):
    steps, sentences, units = tokens.shape
    depth, width = w_input.shape[1:]
    groups = lax.axis_size("col") // 2
    half = sentences // 2
    bf16, f32, dma = jnp.bfloat16, jnp.float32, pltpu.SemaphoreType.DMA
    vmem = pl.BlockSpec(memory_space=pltpu.VMEM)
    return pl.pallas_call(
        functools.partial(lstm_kernel, groups),
        out_shape=(
            jax.ShapeDtypeStruct((steps // 2, sentences, units), bf16),
            jax.ShapeDtypeStruct((1, sentences, units), bf16),
            jax.ShapeDtypeStruct((1, sentences, units), f32),
        ),
        in_specs=[pl.BlockSpec(memory_space=pl.ANY)] * 3 + [vmem],
        out_specs=(vmem, vmem, vmem),
        scratch_shapes=[
            pltpu.VMEM((steps, groups, 2, half, units), bf16),
            pltpu.VMEM((steps, groups, 2, half, units), bf16),
            pltpu.VMEM((steps // 2, groups, 2, half, units), bf16),
            pltpu.VMEM((2, depth, width), bf16),
            pltpu.VMEM((2, depth, width), bf16),
            pltpu.VMEM((depth, width), bf16),
            pltpu.VMEM((depth, width), bf16),
            pltpu.VMEM((depth, width), bf16),
            pltpu.VMEM((depth, width), bf16),
            pltpu.VMEM((1, width), f32),
            pltpu.VMEM((2, 8, width), f32),
            pltpu.VMEM((2, half, units), f32),
            pltpu.VMEM((2, half, width), f32),
            dma,
            dma((steps, groups)),
            dma((steps, groups)),
            dma((steps // CHUNK // 2,)),
            dma((steps // CHUNK // 2, groups, 2)),
            dma((steps // CHUNK // 2,)),
            dma((steps // CHUNK // 2,)),
            dma((2,)),
            dma((2,)),
            dma((2,)),
            dma,
            dma((steps // 2, 2)),
            dma((2,)),
        ],
        compiler_params=pltpu.CompilerParams(
            collective_id=0, has_side_effects=True, vmem_limit_bytes=48 * 2**20
        ),
        name="lstm",
    )(tokens, w_input[0], w_recur[0], bias)


def solution(mesh):
    in_specs = (
        P(None, "dp", "col"),
        P("layer", None, "col"),
        P("layer", None, "col"),
        P("layer", "col"),
    )
    out_specs = (P("layer", "dp", "col"), P("layer", "dp", "col"), P("layer", "dp", "col"))
    cols = mesh.shape["col"]

    def body(tokens, w_input, w_recur, bias):
        steps, sentences, units = tokens.shape
        fits = mesh.shape["layer"] == 2 and mesh.shape["dp"] == 2 and cols % 2 == 0
        fits = fits and units % 128 == 0 and sentences % 32 == 0 and steps % (2 * CHUNK) == 0
        return (fused if fits else shards)(tokens, w_input, w_recur, bias)

    return jax.shard_map(body, mesh=mesh, in_specs=in_specs, out_specs=out_specs, check_vma=False)
```

```python
import functools

import jax
import jax.numpy as jnp
from jax import lax
from jax.experimental import pallas as pl
from jax.experimental.pallas import tpu as pltpu
from jax.sharding import PartitionSpec as P


def passed_along(block, axis, distance):
    devices = range(lax.axis_size(axis))
    route = [(i - distance, i) for i in devices if i - distance in devices]
    return lax.ppermute(block, axis, route)


def broadcast(block, axis, source):
    block = jnp.where(lax.axis_index(axis) == source, block, jnp.zeros_like(block))
    return lax.psum(block, axis)


def shards(tokens, w_input, w_recur, bias):
    steps_count, sentences, units = tokens.shape
    w_local = w_input[0]
    r_local = w_recur[0]
    b_local = bias[0]
    layers = lax.axis_size("layer")
    level = lax.axis_index("layer")
    is_first = level == 0
    has_skip = level >= 1
    is_last = level == layers - 1

    def cell_step(gates, cell):
        gates = gates.reshape(sentences, units, 4)
        in_gate = jax.nn.sigmoid(gates[:, :, 0])
        forget = jax.nn.sigmoid(gates[:, :, 1])
        update = jnp.tanh(gates[:, :, 2])
        out_gate = jax.nn.sigmoid(gates[:, :, 3])
        cell_new = forget * cell + in_gate * update
        hidden_new = (out_gate * jnp.tanh(cell_new)).astype(jnp.bfloat16)
        return (hidden_new, cell_new)

    def skip_sum(hidden_new, in_part):
        summed = (hidden_new.astype(jnp.float32) + in_part.astype(jnp.float32)).astype(jnp.bfloat16)
        return jnp.where(has_skip, summed, hidden_new)

    zero_h = jnp.zeros((sentences, units), jnp.bfloat16)
    zero_c = jnp.zeros((sentences, units), jnp.float32)
    buffer = jnp.zeros((steps_count, sentences, units), jnp.bfloat16)
    span = 4
    count = steps_count // span
    block_sections = count + layers - 1
    zero_span = jnp.zeros((span, sentences, units), jnp.bfloat16)

    def section_block(section, carry):
        hidden, cell, outgoing, kept = carry
        which = section - level
        active = (which >= 0) & (which < count)
        first_step = jnp.clip(which, 0, count - 1) * span
        own_tokens = lax.dynamic_slice_in_dim(tokens, first_step, span, 0)
        received = passed_along(outgoing, "layer", 1)
        in_part = jnp.where(is_first, own_tokens, received)
        in_full = lax.all_gather(in_part, "col", axis=2, tiled=True)
        projected = jnp.dot(
            in_full.reshape(span * sentences, in_full.shape[2]),
            w_local,
            preferred_element_type=jnp.float32,
        )
        projected = projected.reshape(span, sentences, w_local.shape[1])
        states = []
        for offset in range(span):
            h_full = lax.all_gather(hidden, "col", axis=1, tiled=True)
            gates = (
                projected[offset]
                + jnp.dot(h_full, r_local, preferred_element_type=jnp.float32)
                + b_local
            )
            hidden_new, cell_new = cell_step(gates, cell)
            hidden = jnp.where(active, hidden_new, hidden)
            cell = jnp.where(active, cell_new, cell)
            states.append(hidden_new)
        produced = jnp.stack(states)
        outgoing = skip_sum(produced, in_part)
        written = lax.dynamic_update_slice_in_dim(kept, produced, first_step, 0)
        kept = jnp.where(active & is_last, written, kept)
        return (hidden, cell, outgoing, kept)

    hidden, cell, outgoing, buffer = lax.fori_loop(
        0, block_sections, section_block, (zero_h, zero_c, zero_span, buffer)
    )
    everything = broadcast(buffer, "layer", layers - 1)
    block = steps_count // layers
    top_states = lax.dynamic_slice_in_dim(everything, level * block, block, 0)
    return (top_states, hidden[None], cell[None])


MESH = pl.DeviceIdType.MESH
CHUNK = 4
SUBS = 2


def lstm_kernel(
    groups,
    tokens, w_in, w_rec, bias,
    top, final_h, final_c,
    xs, hs, ts, wi, wr, own_in, own_rec, raw_in, raw_rec, braw, bperm, cell, gates,
    send_sem, x_sem, h_sem, tok_y_sem, tok_z_sem, tok_x_sem, tok_own_sem,
    w_own_sem, w_y_sem, w_d_sem, b_sem, top_sem, fin_sem,
):
    steps, sentences, units = tokens.shape
    half = sentences // 2
    sub = half // SUBS
    depth = w_in.shape[0]
    part_rows = depth // 2
    keep = steps // 2
    chunks = keep // CHUNK
    dp = lax.axis_index("dp")
    level = lax.axis_index("layer")
    col = lax.axis_index("col")
    p = col // 2
    q = lax.rem(col, 2)
    other = 1 - q
    pair = {"col": 2 * p + other}
    twin = {"dp": 1 - dp}
    is_first = level == 0
    is_last = level == 1

    def copy(src, dst, sem, device):
        return pltpu.make_async_remote_copy(
            src_ref=src, dst_ref=dst, send_sem=send_sem, recv_sem=sem,
            device_id=device, device_id_type=MESH,
        )

    def near(i):
        return lax.rem(p + i, groups)

    def nearest(i):
        ranks = [sorted((abs(g - k), g) for g in range(groups))[i][1] for k in range(groups)]
        return sum(jnp.where(p == k, g, 0) for k, g in enumerate(ranks))

    peers = [nearest(i) for i in range(1, groups)]

    barrier = pltpu.get_barrier_semaphore()
    targets = [{"col": 2 * near(i) + q} for i in range(1, groups)]
    targets += [pair, twin]
    targets += [{"layer": 1 - level, "col": 2 * p + y} for y in range(2)]
    for device in targets:
        pl.semaphore_signal(barrier, inc=1, device_id=device, device_id_type=MESH)
    pl.semaphore_wait(barrier, len(targets))

    my_rows = pl.ds(pl.multiple_of(q * half, half), half)
    other_rows = pl.ds(pl.multiple_of(other * half, half), half)

    def span(c):
        return pl.ds(c * CHUNK, CHUNK)

    def source(c):
        return pl.ds(level * keep + c * CHUNK, CHUNK)

    def tok_local(buf, c):
        return pltpu.make_async_copy(tokens.at[source(c), my_rows], buf.at[span(c), p, q], tok_own_sem.at[c])

    def tok_to_pair(buf, c):
        return copy(tokens.at[source(c), other_rows], buf.at[span(c), p, q], tok_y_sem.at[c], pair)

    def tok_from_pair(buf, c):
        place = buf.at[span(c), p, other]
        return copy(place, place, tok_y_sem.at[c], pair)

    def tok_own(buf, c, i):
        return copy(tokens.at[source(c), my_rows], buf.at[span(c), p, q], tok_z_sem.at[c, p, q], {"col": 2 * near(i) + q})

    def tok_forward(buf, c, i):
        place = buf.at[span(c), p, other]
        return copy(place, place, tok_z_sem.at[c, p, other], {"col": 2 * near(i) + q})

    def tok_arrived(buf, c, i, y):
        place = buf.at[span(c), near(i), y]
        return copy(place, place, tok_z_sem.at[c, near(i), y], pair)

    def tok_over(c):
        return copy(ts.at[span(c)], xs.at[pl.ds(keep + c * CHUNK, CHUNK)], tok_x_sem.at[c], {"layer": 1 - level})

    def tok_all(buf, c):
        for i in range(1, groups):
            tok_arrived(buf, c, i, 0).wait_recv()
            tok_arrived(buf, c, i, 1).wait_recv()

    part = pl.ds(pl.multiple_of(dp * part_rows, part_rows), part_rows)
    twin_part = pl.ds(pl.multiple_of((1 - dp) * part_rows, part_rows), part_rows)
    weights = ((w_in, raw_in), (w_rec, raw_rec))

    def w_to_pair(k):
        own, raw = weights[k]
        return copy(own.at[part], raw.at[part], w_y_sem.at[k], pair)

    def w_to_twin(k):
        raw = weights[k][1]
        return copy(raw.at[part], raw.at[part], w_d_sem.at[k], twin)

    def w_from_twin(k):
        raw = weights[k][1]
        return copy(raw.at[twin_part], raw.at[twin_part], w_d_sem.at[k], twin)

    bias_copy = copy(bias, braw, b_sem, pair)

    def own_weights(k):
        return pltpu.make_async_copy(weights[k][0], (own_in, own_rec)[k], w_own_sem.at[k])

    @pl.when(is_first)
    def _():
        tok_to_pair(xs, 0).start()
        for i in range(1, groups):
            tok_own(xs, 0, i).start()

    @pl.when(is_last)
    def _():
        for c in range(chunks):
            tok_to_pair(ts, c).start()
        for i in range(1, groups):
            tok_own(ts, 0, i).start()

    own_weights(0).start()
    bias_copy.start()
    w_to_pair(0).start()

    @pl.when(is_first)
    def _():
        for c in range(1, chunks):
            tok_to_pair(xs, c).start()
        for c in range(chunks):
            tok_local(xs, c).start()

    @pl.when(is_last)
    def _():
        for c in range(chunks):
            tok_local(ts, c).start()

    own_weights(1).start()
    w_to_pair(1).start()

    cell[...] = jnp.zeros_like(cell)
    width = 4 * units
    row = lax.broadcasted_iota(jnp.int32, (width, width), 0)
    column = lax.broadcasted_iota(jnp.int32, (width, width), 1)
    spread = row == 4 * lax.rem(column, units) + column // units
    order = jnp.where(spread, 1.0, 0.0).astype(jnp.bfloat16)
    block_rows = 256

    def regroup(src, dst, which):
        @pl.loop(0, depth // block_rows)
        def _(r):
            rows = pl.ds(pl.multiple_of(r * block_rows, block_rows), block_rows)
            moved = jnp.dot(src[rows], order, preferred_element_type=jnp.float32)
            dst[which, rows] = moved.astype(jnp.bfloat16)

    def regroup_bias(src, which):
        value = jnp.broadcast_to(src[...], (8, width))
        total = jnp.zeros((8, width), jnp.float32)
        for _ in range(3):
            piece = value.astype(jnp.bfloat16)
            total = total + jnp.dot(piece, order, preferred_element_type=jnp.float32)
            value = value - piece.astype(jnp.float32)
        bperm[which] = total

    own_weights(0).wait()
    regroup(own_in, wi, q)
    regroup_bias(bias, q)

    def hand_on(buf):
        for c in range(chunks):
            tok_from_pair(buf, c).wait_recv()
            for i in range(1, groups):
                tok_forward(buf, c, i).start()
            if c + 1 < chunks:
                for i in range(1, groups):
                    tok_own(buf, c + 1, i).start()

    @pl.when(is_last)
    def _():
        hand_on(ts)

    @pl.when(is_first)
    def _():
        tok_from_pair(xs, 0).wait_recv()
        for i in range(1, groups):
            tok_forward(xs, 0, i).start()
        for c in range(1, chunks):
            for i in range(1, groups):
                tok_own(xs, c, i).start()

    own_weights(1).wait()
    regroup(own_rec, wr, q)
    bias_copy.wait_recv()
    regroup_bias(braw, other)
    w_to_pair(0).wait_recv()
    w_to_twin(0).start()
    w_from_twin(0).wait_recv()
    regroup(raw_in, wi, other)

    @pl.when(is_first)
    def _():
        for c in range(1, chunks):
            tok_from_pair(xs, c).wait_recv()
            for i in range(1, groups):
                tok_forward(xs, c, i).start()

    @pl.when(is_last)
    def _():
        for c in range(chunks):
            tok_local(ts, c).wait()
            tok_all(ts, c)
            tok_over(c).start()

    def to_peer(t, s, g):
        return copy(hs.at[t, p, s], hs.at[t, p, s], h_sem.at[t, p, s], {"col": 2 * g + q})

    def from_peer(t, s, g):
        return copy(hs.at[t, g, s], hs.at[t, g, s], h_sem.at[t, g, s], pair)

    def sub_rows(s):
        return pl.ds(s * sub, sub)

    def out_rows(y, s):
        return pl.ds(pl.multiple_of(y * half + s * sub, sub), sub)

    def to_next(t, s, g):
        return copy(hs.at[t, g, s], xs.at[t, g, :, sub_rows(s)], x_sem.at[t, g, s], {"layer": 1 - level})

    def joined(ref, t):
        return jnp.concatenate([ref[t, g, y] for g in range(groups) for y in range(2)], axis=1)

    def top_far(t, s, b):
        return copy(hs.at[t, p, s, b], top.at[t, out_rows(q, s)], top_sem.at[t, q, s], {"layer": 1 - level, "col": 2 * p + b})

    def top_pair(t, s):
        return copy(hs.at[t, p, s, other], top.at[t - keep, out_rows(q, s)], top_sem.at[t - keep, q, s], pair)

    def top_in(t, y, s):
        rows = top.at[t, out_rows(y, s)]
        return copy(rows, rows, top_sem.at[t, y, s], pair)

    def add_recurrent(t, s, g):
        state = jnp.concatenate([hs[t, g, s, 0], hs[t, g, s, 1]], axis=1)
        rows = pl.ds(pl.multiple_of(g * 2 * units, 2 * units), 2 * units)
        for b in range(2):
            gates[b, sub_rows(s)] += jnp.dot(state, wr[b, rows], preferred_element_type=jnp.float32)

    def peer_in(t, s, g):
        from_peer(t, s, g).wait_recv()

        @pl.when(is_first)
        def _():
            to_next(t, s, g).start()

    @pl.loop(0, steps)
    def _(t):
        @pl.when(is_first & (lax.rem(t, CHUNK) == 0))
        def _():
            c = lax.rem(t // CHUNK, chunks)

            @pl.when(t < keep)
            def _():
                tok_local(xs, c).wait()
                tok_all(xs, c)

            @pl.when(t >= keep)
            def _():
                tok_over(c).wait_recv()

        @pl.when(is_last)
        def _():
            for g in range(groups):
                for s in range(SUBS):
                    to_next(t, s, g).wait_recv()

        given = joined(xs, t)
        for b in range(2):
            gates[b] = jnp.dot(given, wi[b], preferred_element_type=jnp.float32) + bperm[b, 0:1]

        @pl.when(t == 1)
        def _():
            w_to_pair(1).wait_recv()
            w_to_twin(1).start()
            w_from_twin(1).wait_recv()
            regroup(raw_rec, wr, other)

        @pl.when(t > 0)
        def _():
            for s in range(SUBS):
                add_recurrent(t - 1, s, p)

        for s in range(SUBS):
            rows = sub_rows(s)

            @pl.when(t > 0)
            def _():
                for g in peers:
                    peer_in(t - 1, s, g)
                    add_recurrent(t - 1, s, g)

            for b in range(2):
                in_gate = 0.5 * jnp.tanh(0.5 * gates[b, rows, 0:units]) + 0.5
                forget = 0.5 * jnp.tanh(0.5 * gates[b, rows, units : 2 * units]) + 0.5
                update = jnp.tanh(gates[b, rows, 2 * units : 3 * units])
                out_gate = 0.5 * jnp.tanh(0.5 * gates[b, rows, 3 * units :]) + 0.5
                cell_new = forget * cell[b, rows] + in_gate * update
                cell[b, rows] = cell_new
                hs[t, p, s, b] = (out_gate * jnp.tanh(cell_new)).astype(jnp.bfloat16)

            @pl.when(is_first | (t < steps - 1))
            def _():
                for g in reversed(peers):
                    to_peer(t, s, g).start()

            @pl.when(is_first)
            def _():
                to_next(t, s, p).start()

            @pl.when(is_last & (t < keep))
            def _():
                top_far(t, s, 0).start()
                top_far(t, s, 1).start()

            @pl.when(is_last & (t >= keep))
            def _():
                top_pair(t, s).start()
                top[t - keep, out_rows(q, s)] = hs[t, p, s, q]

    end = steps - 1

    @pl.when(is_first)
    def _():
        for s in range(SUBS):
            for g in peers:
                peer_in(end, s, g)

    def fin_h(s):
        return copy(hs.at[end, p, s, other], final_h.at[0, out_rows(q, s)], fin_sem.at[1 + s], pair)

    fin_c = copy(cell.at[other], final_c.at[0, my_rows], fin_sem.at[0], pair)
    fin_c.start()
    final_c[0, my_rows] = cell[q]
    for s in range(SUBS):
        fin_h(s).start()
        final_h[0, out_rows(q, s)] = hs[end, p, s, q]

    bias_copy.wait_send()
    for k in range(2):
        w_to_pair(k).wait_send()
        w_to_twin(k).wait_send()
    fin_c.wait()
    for s in range(SUBS):
        fin_h(s).wait()

    @pl.loop(0, end)
    def _(t):
        for s in range(SUBS):
            for g in peers:
                to_peer(t, s, g).wait_send()

    def tokens_sent(buf):
        for c in range(chunks):
            tok_to_pair(buf, c).wait_send()
            for i in range(1, groups):
                tok_own(buf, c, i).wait_send()
                tok_forward(buf, c, i).wait_send()

    @pl.when(is_first)
    def _():
        tokens_sent(xs)
        for s in range(SUBS):
            for g in peers:
                to_peer(end, s, g).wait_send()

        @pl.loop(0, steps)
        def _(t):
            for s in range(SUBS):
                for g in range(groups):
                    to_next(t, s, g).wait_send()

        @pl.loop(0, keep)
        def _(t):
            for s in range(SUBS):
                for y in range(2):
                    top_in(t, y, s).wait_recv()

    @pl.when(is_last)
    def _():
        tokens_sent(ts)
        for c in range(chunks):
            tok_over(c).wait_send()

        @pl.loop(0, keep)
        def _(t):
            for s in range(SUBS):
                top_far(t, s, 0).wait_send()
                top_far(t, s, 1).wait_send()
                top_pair(t + keep, s).wait_send()
                top_in(t, other, s).wait_recv()


def fused(tokens, w_input, w_recur, bias):
    steps, sentences, units = tokens.shape
    depth, width = w_input.shape[1:]
    groups = lax.axis_size("col") // 2
    half = sentences // 2
    bf16, f32, dma = jnp.bfloat16, jnp.float32, pltpu.SemaphoreType.DMA
    vmem = pl.BlockSpec(memory_space=pltpu.VMEM)
    return pl.pallas_call(
        functools.partial(lstm_kernel, groups),
        out_shape=(
            jax.ShapeDtypeStruct((steps // 2, sentences, units), bf16),
            jax.ShapeDtypeStruct((1, sentences, units), bf16),
            jax.ShapeDtypeStruct((1, sentences, units), f32),
        ),
        in_specs=[pl.BlockSpec(memory_space=pltpu.HBM)] * 3 + [vmem],
        out_specs=(vmem, vmem, vmem),
        scratch_shapes=[
            pltpu.VMEM((steps, groups, 2, half, units), bf16),
            pltpu.VMEM((steps, groups, SUBS, 2, half // SUBS, units), bf16),
            pltpu.VMEM((steps // 2, groups, 2, half, units), bf16),
            pltpu.VMEM((2, depth, width), bf16),
            pltpu.VMEM((2, depth, width), bf16),
            pltpu.VMEM((depth, width), bf16),
            pltpu.VMEM((depth, width), bf16),
            pltpu.VMEM((depth, width), bf16),
            pltpu.VMEM((depth, width), bf16),
            pltpu.VMEM((1, width), f32),
            pltpu.VMEM((2, 8, width), f32),
            pltpu.VMEM((2, half, units), f32),
            pltpu.VMEM((2, half, width), f32),
            dma,
            dma((steps, groups, SUBS)),
            dma((steps, groups, SUBS)),
            dma((steps // CHUNK // 2,)),
            dma((steps // CHUNK // 2, groups, 2)),
            dma((steps // CHUNK // 2,)),
            dma((steps // CHUNK // 2,)),
            dma((2,)),
            dma((2,)),
            dma((2,)),
            dma,
            dma((steps // 2, 2, SUBS)),
            dma((1 + SUBS,)),
        ],
        compiler_params=pltpu.CompilerParams(
            collective_id=0, has_side_effects=True, vmem_limit_bytes=67_000_000
        ),
        name="lstm",
    )(tokens, w_input[0], w_recur[0], bias)


def solution(mesh):
    in_specs = (
        P(None, "dp", "col"),
        P("layer", None, "col"),
        P("layer", None, "col"),
        P("layer", "col"),
    )
    out_specs = (P("layer", "dp", "col"), P("layer", "dp", "col"), P("layer", "dp", "col"))
    cols = mesh.shape["col"]

    def body(tokens, w_input, w_recur, bias):
        steps, sentences, units = tokens.shape
        fits = mesh.shape["layer"] == 2 and mesh.shape["dp"] == 2 and cols % 2 == 0
        fits = fits and units % 128 == 0 and sentences % (32 * SUBS) == 0 and steps % (2 * CHUNK) == 0
        return (fused if fits else shards)(tokens, w_input, w_recur, bias)

    return jax.shard_map(body, mesh=mesh, in_specs=in_specs, out_specs=out_specs, check_vma=False)
```

```python
import functools

import jax
import jax.numpy as jnp
from jax import lax
from jax.experimental import pallas as pl
from jax.experimental.pallas import tpu as pltpu
from jax.sharding import PartitionSpec as P


def passed_along(block, axis, distance):
    devices = range(lax.axis_size(axis))
    route = [(i - distance, i) for i in devices if i - distance in devices]
    return lax.ppermute(block, axis, route)


def broadcast(block, axis, source):
    block = jnp.where(lax.axis_index(axis) == source, block, jnp.zeros_like(block))
    return lax.psum(block, axis)


def shards(tokens, w_input, w_recur, bias):
    steps_count, sentences, units = tokens.shape
    w_local = w_input[0]
    r_local = w_recur[0]
    b_local = bias[0]
    layers = lax.axis_size("layer")
    level = lax.axis_index("layer")
    is_first = level == 0
    has_skip = level >= 1
    is_last = level == layers - 1

    def cell_step(gates, cell):
        gates = gates.reshape(sentences, units, 4)
        in_gate = jax.nn.sigmoid(gates[:, :, 0])
        forget = jax.nn.sigmoid(gates[:, :, 1])
        update = jnp.tanh(gates[:, :, 2])
        out_gate = jax.nn.sigmoid(gates[:, :, 3])
        cell_new = forget * cell + in_gate * update
        hidden_new = (out_gate * jnp.tanh(cell_new)).astype(jnp.bfloat16)
        return (hidden_new, cell_new)

    def skip_sum(hidden_new, in_part):
        summed = (hidden_new.astype(jnp.float32) + in_part.astype(jnp.float32)).astype(jnp.bfloat16)
        return jnp.where(has_skip, summed, hidden_new)

    zero_h = jnp.zeros((sentences, units), jnp.bfloat16)
    zero_c = jnp.zeros((sentences, units), jnp.float32)
    buffer = jnp.zeros((steps_count, sentences, units), jnp.bfloat16)
    span = 4
    count = steps_count // span
    block_sections = count + layers - 1
    zero_span = jnp.zeros((span, sentences, units), jnp.bfloat16)

    def section_block(section, carry):
        hidden, cell, outgoing, kept = carry
        which = section - level
        active = (which >= 0) & (which < count)
        first_step = jnp.clip(which, 0, count - 1) * span
        own_tokens = lax.dynamic_slice_in_dim(tokens, first_step, span, 0)
        received = passed_along(outgoing, "layer", 1)
        in_part = jnp.where(is_first, own_tokens, received)
        in_full = lax.all_gather(in_part, "col", axis=2, tiled=True)
        projected = jnp.dot(
            in_full.reshape(span * sentences, in_full.shape[2]),
            w_local,
            preferred_element_type=jnp.float32,
        )
        projected = projected.reshape(span, sentences, w_local.shape[1])
        states = []
        for offset in range(span):
            h_full = lax.all_gather(hidden, "col", axis=1, tiled=True)
            gates = (
                projected[offset]
                + jnp.dot(h_full, r_local, preferred_element_type=jnp.float32)
                + b_local
            )
            hidden_new, cell_new = cell_step(gates, cell)
            hidden = jnp.where(active, hidden_new, hidden)
            cell = jnp.where(active, cell_new, cell)
            states.append(hidden_new)
        produced = jnp.stack(states)
        outgoing = skip_sum(produced, in_part)
        written = lax.dynamic_update_slice_in_dim(kept, produced, first_step, 0)
        kept = jnp.where(active & is_last, written, kept)
        return (hidden, cell, outgoing, kept)

    hidden, cell, outgoing, buffer = lax.fori_loop(
        0, block_sections, section_block, (zero_h, zero_c, zero_span, buffer)
    )
    everything = broadcast(buffer, "layer", layers - 1)
    block = steps_count // layers
    top_states = lax.dynamic_slice_in_dim(everything, level * block, block, 0)
    return (top_states, hidden[None], cell[None])


MESH = pl.DeviceIdType.MESH
CHUNK = 4
SUBS = 2
PIECES = 2


def lstm_kernel(
    groups,
    tokens, w_in, w_rec, bias,
    top, final_h, final_c,
    xs, hs, ts, wi, wr, own_in, own_rec, raw_in, raw_rec, braw, bperm, cell, gates,
    send_sem, x_sem, h_sem, tok_y_sem, tok_z_sem, tok_x_sem, tok_own_sem,
    w_own_sem, w_y_sem, w_d_sem, b_sem, top_sem, fin_sem,
):
    steps, sentences, units = tokens.shape
    half = sentences // 2
    sub = half // SUBS
    depth = w_in.shape[0]
    part_rows = depth // 2
    keep = steps // 2
    chunks = keep // CHUNK
    dp = lax.axis_index("dp")
    level = lax.axis_index("layer")
    col = lax.axis_index("col")
    p = col // 2
    q = lax.rem(col, 2)
    other = 1 - q
    pair = {"col": 2 * p + other}
    twin = {"dp": 1 - dp}
    is_first = level == 0
    is_last = level == 1

    def copy(src, dst, sem, device):
        return pltpu.make_async_remote_copy(
            src_ref=src, dst_ref=dst, send_sem=send_sem, recv_sem=sem,
            device_id=device, device_id_type=MESH,
        )

    def near(i):
        return lax.rem(p + i, groups)

    def nearest(i):
        ranks = [sorted((abs(g - k), g) for g in range(groups))[i][1] for k in range(groups)]
        return sum(jnp.where(p == k, g, 0) for k, g in enumerate(ranks))

    peers = [nearest(i) for i in range(1, groups)]

    barrier = pltpu.get_barrier_semaphore()
    targets = [{"col": 2 * near(i) + q} for i in range(1, groups)]
    targets += [pair, twin]
    targets += [{"layer": 1 - level, "col": 2 * p + y} for y in range(2)]
    for device in targets:
        pl.semaphore_signal(barrier, inc=1, device_id=device, device_id_type=MESH)
    pl.semaphore_wait(barrier, len(targets))

    my_rows = pl.ds(pl.multiple_of(q * half, half), half)
    other_rows = pl.ds(pl.multiple_of(other * half, half), half)

    def span(c):
        return pl.ds(c * CHUNK, CHUNK)

    def source(c):
        return pl.ds(level * keep + c * CHUNK, CHUNK)

    def tok_local(buf, c):
        return pltpu.make_async_copy(tokens.at[source(c), my_rows], buf.at[span(c), p, q], tok_own_sem.at[c])

    def tok_to_pair(buf, c):
        return copy(tokens.at[source(c), other_rows], buf.at[span(c), p, q], tok_y_sem.at[c], pair)

    def tok_from_pair(buf, c):
        place = buf.at[span(c), p, other]
        return copy(place, place, tok_y_sem.at[c], pair)

    def tok_own(buf, c, i):
        return copy(tokens.at[source(c), my_rows], buf.at[span(c), p, q], tok_z_sem.at[c, p, q], {"col": 2 * near(i) + q})

    def tok_forward(buf, c, i):
        place = buf.at[span(c), p, other]
        return copy(place, place, tok_z_sem.at[c, p, other], {"col": 2 * near(i) + q})

    def tok_arrived(buf, c, i, y):
        place = buf.at[span(c), near(i), y]
        return copy(place, place, tok_z_sem.at[c, near(i), y], pair)

    def tok_over(c):
        return copy(ts.at[span(c)], xs.at[pl.ds(keep + c * CHUNK, CHUNK)], tok_x_sem.at[c], {"layer": 1 - level})

    def tok_all(buf, c):
        for i in range(1, groups):
            tok_arrived(buf, c, i, 0).wait_recv()
            tok_arrived(buf, c, i, 1).wait_recv()

    weights = ((w_in, raw_in), (w_rec, raw_rec))
    piece_rows = part_rows // PIECES

    def piece(core, n):
        return pl.ds(pl.multiple_of(core * part_rows + n * piece_rows, piece_rows), piece_rows)

    def w_to_pair(k, n):
        own, raw = weights[k]
        return copy(own.at[piece(dp, n)], raw.at[piece(dp, n)], w_y_sem.at[k, n], pair)

    def w_to_twin(k, n):
        raw = weights[k][1]
        return copy(raw.at[piece(dp, n)], raw.at[piece(dp, n)], w_d_sem.at[k, n], twin)

    def w_from_twin(k, n):
        raw = weights[k][1]
        return copy(raw.at[piece(1 - dp, n)], raw.at[piece(1 - dp, n)], w_d_sem.at[k, n], twin)

    bias_copy = copy(bias, braw, b_sem, pair)

    def own_weights(k):
        return pltpu.make_async_copy(weights[k][0], (own_in, own_rec)[k], w_own_sem.at[k])

    @pl.when(is_first)
    def _():
        tok_to_pair(xs, 0).start()
        for i in range(1, groups):
            tok_own(xs, 0, i).start()

    @pl.when(is_last)
    def _():
        for c in range(chunks):
            tok_to_pair(ts, c).start()
        for i in range(1, groups):
            tok_own(ts, 0, i).start()

    own_weights(0).start()
    bias_copy.start()
    for n in range(PIECES):
        w_to_pair(0, n).start()

    @pl.when(is_first)
    def _():
        for c in range(1, chunks):
            tok_to_pair(xs, c).start()
        for c in range(chunks):
            tok_local(xs, c).start()

    @pl.when(is_last)
    def _():
        for c in range(chunks):
            tok_local(ts, c).start()

    own_weights(1).start()

    cell[...] = jnp.zeros_like(cell)
    width = 4 * units
    row = lax.broadcasted_iota(jnp.int32, (width, width), 0)
    column = lax.broadcasted_iota(jnp.int32, (width, width), 1)
    spread = row == 4 * lax.rem(column, units) + column // units
    order = jnp.where(spread, 1.0, 0.0).astype(jnp.bfloat16)
    block_rows = 256

    def regroup(src, dst, which):
        @pl.loop(0, depth // block_rows)
        def _(r):
            rows = pl.ds(pl.multiple_of(r * block_rows, block_rows), block_rows)
            moved = jnp.dot(src[rows], order, preferred_element_type=jnp.float32)
            dst[which, rows] = moved.astype(jnp.bfloat16)

    def regroup_piece(src, dst, rows):
        moved = jnp.dot(src[rows], order, preferred_element_type=jnp.float32)
        dst[other, rows] = moved.astype(jnp.bfloat16)

    def swap_weights(k, dst):
        raw = weights[k][1]
        for n in range(PIECES):
            w_to_pair(k, n).wait_recv()
            w_to_twin(k, n).start()
            if k == 0:
                w_to_pair(1, n).start()
            regroup_piece(raw, dst, piece(dp, n))
        for n in range(PIECES):
            w_from_twin(k, n).wait_recv()
            regroup_piece(raw, dst, piece(1 - dp, n))

    def regroup_bias(src, which):
        value = jnp.broadcast_to(src[...], (8, width))
        total = jnp.zeros((8, width), jnp.float32)
        for _ in range(3):
            piece = value.astype(jnp.bfloat16)
            total = total + jnp.dot(piece, order, preferred_element_type=jnp.float32)
            value = value - piece.astype(jnp.float32)
        bperm[which] = total

    own_weights(0).wait()
    regroup(own_in, wi, q)
    regroup_bias(bias, q)

    def hand_on(buf):
        for c in range(chunks):
            tok_from_pair(buf, c).wait_recv()
            for i in range(1, groups):
                tok_forward(buf, c, i).start()
            if c + 1 < chunks:
                for i in range(1, groups):
                    tok_own(buf, c + 1, i).start()

    @pl.when(is_last)
    def _():
        hand_on(ts)

    @pl.when(is_first)
    def _():
        tok_from_pair(xs, 0).wait_recv()
        for i in range(1, groups):
            tok_forward(xs, 0, i).start()
        for c in range(1, chunks):
            for i in range(1, groups):
                tok_own(xs, c, i).start()

    own_weights(1).wait()
    regroup(own_rec, wr, q)
    bias_copy.wait_recv()
    regroup_bias(braw, other)
    swap_weights(0, wi)

    @pl.when(is_first)
    def _():
        for c in range(1, chunks):
            tok_from_pair(xs, c).wait_recv()
            for i in range(1, groups):
                tok_forward(xs, c, i).start()

    @pl.when(is_last)
    def _():
        for c in range(chunks):
            tok_local(ts, c).wait()
            tok_all(ts, c)
            tok_over(c).start()

    def to_peer(t, s, g):
        return copy(hs.at[t, p, s], hs.at[t, p, s], h_sem.at[t, p, s], {"col": 2 * g + q})

    def from_peer(t, s, g):
        return copy(hs.at[t, g, s], hs.at[t, g, s], h_sem.at[t, g, s], pair)

    def sub_rows(s):
        return pl.ds(s * sub, sub)

    def out_rows(y, s):
        return pl.ds(pl.multiple_of(y * half + s * sub, sub), sub)

    def to_next(t, s, g):
        return copy(hs.at[t, g, s], xs.at[t, g, :, sub_rows(s)], x_sem.at[t, g, s], {"layer": 1 - level})

    def joined(ref, t):
        return jnp.concatenate([ref[t, g, y] for g in range(groups) for y in range(2)], axis=1)

    def top_far(t, s, b):
        return copy(hs.at[t, p, s, b], top.at[t, out_rows(q, s)], top_sem.at[t, q, s], {"layer": 1 - level, "col": 2 * p + b})

    def top_pair(t, s):
        return copy(hs.at[t, p, s, other], top.at[t - keep, out_rows(q, s)], top_sem.at[t - keep, q, s], pair)

    def top_in(t, y, s):
        rows = top.at[t, out_rows(y, s)]
        return copy(rows, rows, top_sem.at[t, y, s], pair)

    def add_recurrent(t, s, g):
        state = jnp.concatenate([hs[t, g, s, 0], hs[t, g, s, 1]], axis=1)
        rows = pl.ds(pl.multiple_of(g * 2 * units, 2 * units), 2 * units)
        for b in range(2):
            gates[b, sub_rows(s)] += jnp.dot(state, wr[b, rows], preferred_element_type=jnp.float32)

    def peer_in(t, s, g):
        from_peer(t, s, g).wait_recv()

        @pl.when(is_first)
        def _():
            to_next(t, s, g).start()

    @pl.loop(0, steps)
    def _(t):
        @pl.when(is_first & (lax.rem(t, CHUNK) == 0))
        def _():
            c = lax.rem(t // CHUNK, chunks)

            @pl.when(t < keep)
            def _():
                tok_local(xs, c).wait()
                tok_all(xs, c)

            @pl.when(t >= keep)
            def _():
                tok_over(c).wait_recv()

        @pl.when(is_last)
        def _():
            for g in range(groups):
                for s in range(SUBS):
                    to_next(t, s, g).wait_recv()

        given = joined(xs, t)
        for b in range(2):
            gates[b] = jnp.dot(given, wi[b], preferred_element_type=jnp.float32) + bperm[b, 0:1]

        @pl.when(t == 1)
        def _():
            swap_weights(1, wr)

        @pl.when(t > 0)
        def _():
            for s in range(SUBS):
                add_recurrent(t - 1, s, p)

        for s in range(SUBS):
            rows = sub_rows(s)

            @pl.when(t > 0)
            def _():
                for g in peers:
                    peer_in(t - 1, s, g)
                    add_recurrent(t - 1, s, g)

            for b in range(2):
                in_gate = 0.5 * jnp.tanh(0.5 * gates[b, rows, 0:units]) + 0.5
                forget = 0.5 * jnp.tanh(0.5 * gates[b, rows, units : 2 * units]) + 0.5
                update = jnp.tanh(gates[b, rows, 2 * units : 3 * units])
                out_gate = 0.5 * jnp.tanh(0.5 * gates[b, rows, 3 * units :]) + 0.5
                cell_new = forget * cell[b, rows] + in_gate * update
                cell[b, rows] = cell_new
                hs[t, p, s, b] = (out_gate * jnp.tanh(cell_new)).astype(jnp.bfloat16)

            @pl.when(is_first | (t < steps - 1))
            def _():
                for g in reversed(peers):
                    to_peer(t, s, g).start()

            @pl.when(is_first)
            def _():
                to_next(t, s, p).start()

            @pl.when(is_last & (t < keep))
            def _():
                top_far(t, s, 0).start()
                top_far(t, s, 1).start()

            @pl.when(is_last & (t >= keep))
            def _():
                top_pair(t, s).start()
                top[t - keep, out_rows(q, s)] = hs[t, p, s, q]

    end = steps - 1

    @pl.when(is_first)
    def _():
        for s in range(SUBS):
            for g in peers:
                peer_in(end, s, g)

    def fin_h(s):
        return copy(hs.at[end, p, s, other], final_h.at[0, out_rows(q, s)], fin_sem.at[1 + s], pair)

    fin_c = copy(cell.at[other], final_c.at[0, my_rows], fin_sem.at[0], pair)
    fin_c.start()
    final_c[0, my_rows] = cell[q]
    for s in range(SUBS):
        fin_h(s).start()
        final_h[0, out_rows(q, s)] = hs[end, p, s, q]

    bias_copy.wait_send()
    for k in range(2):
        for n in range(PIECES):
            w_to_pair(k, n).wait_send()
            w_to_twin(k, n).wait_send()
    fin_c.wait()
    for s in range(SUBS):
        fin_h(s).wait()

    @pl.loop(0, end)
    def _(t):
        for s in range(SUBS):
            for g in peers:
                to_peer(t, s, g).wait_send()

    def tokens_sent(buf):
        for c in range(chunks):
            tok_to_pair(buf, c).wait_send()
            for i in range(1, groups):
                tok_own(buf, c, i).wait_send()
                tok_forward(buf, c, i).wait_send()

    @pl.when(is_first)
    def _():
        tokens_sent(xs)
        for s in range(SUBS):
            for g in peers:
                to_peer(end, s, g).wait_send()

        @pl.loop(0, steps)
        def _(t):
            for s in range(SUBS):
                for g in range(groups):
                    to_next(t, s, g).wait_send()

        @pl.loop(0, keep)
        def _(t):
            for s in range(SUBS):
                for y in range(2):
                    top_in(t, y, s).wait_recv()

    @pl.when(is_last)
    def _():
        tokens_sent(ts)
        for c in range(chunks):
            tok_over(c).wait_send()

        @pl.loop(0, keep)
        def _(t):
            for s in range(SUBS):
                top_far(t, s, 0).wait_send()
                top_far(t, s, 1).wait_send()
                top_pair(t + keep, s).wait_send()
                top_in(t, other, s).wait_recv()


def fused(tokens, w_input, w_recur, bias):
    steps, sentences, units = tokens.shape
    depth, width = w_input.shape[1:]
    groups = lax.axis_size("col") // 2
    half = sentences // 2
    bf16, f32, dma = jnp.bfloat16, jnp.float32, pltpu.SemaphoreType.DMA
    vmem = pl.BlockSpec(memory_space=pltpu.VMEM)
    return pl.pallas_call(
        functools.partial(lstm_kernel, groups),
        out_shape=(
            jax.ShapeDtypeStruct((steps // 2, sentences, units), bf16),
            jax.ShapeDtypeStruct((1, sentences, units), bf16),
            jax.ShapeDtypeStruct((1, sentences, units), f32),
        ),
        in_specs=[pl.BlockSpec(memory_space=pltpu.HBM)] * 3 + [vmem],
        out_specs=(vmem, vmem, vmem),
        scratch_shapes=[
            pltpu.VMEM((steps, groups, 2, half, units), bf16),
            pltpu.VMEM((steps, groups, SUBS, 2, half // SUBS, units), bf16),
            pltpu.VMEM((steps // 2, groups, 2, half, units), bf16),
            pltpu.VMEM((2, depth, width), bf16),
            pltpu.VMEM((2, depth, width), bf16),
            pltpu.VMEM((depth, width), bf16),
            pltpu.VMEM((depth, width), bf16),
            pltpu.VMEM((depth, width), bf16),
            pltpu.VMEM((depth, width), bf16),
            pltpu.VMEM((1, width), f32),
            pltpu.VMEM((2, 8, width), f32),
            pltpu.VMEM((2, half, units), f32),
            pltpu.VMEM((2, half, width), f32),
            dma,
            dma((steps, groups, SUBS)),
            dma((steps, groups, SUBS)),
            dma((steps // CHUNK // 2,)),
            dma((steps // CHUNK // 2, groups, 2)),
            dma((steps // CHUNK // 2,)),
            dma((steps // CHUNK // 2,)),
            dma((2,)),
            dma((2, PIECES)),
            dma((2, PIECES)),
            dma,
            dma((steps // 2, 2, SUBS)),
            dma((1 + SUBS,)),
        ],
        compiler_params=pltpu.CompilerParams(
            collective_id=0, has_side_effects=True, vmem_limit_bytes=66_590_000
        ),
        name="lstm",
    )(tokens, w_input[0], w_recur[0], bias)


def solution(mesh):
    in_specs = (
        P(None, "dp", "col"),
        P("layer", None, "col"),
        P("layer", None, "col"),
        P("layer", "col"),
    )
    out_specs = (P("layer", "dp", "col"), P("layer", "dp", "col"), P("layer", "dp", "col"))
    cols = mesh.shape["col"]

    def body(tokens, w_input, w_recur, bias):
        steps, sentences, units = tokens.shape
        fits = mesh.shape["layer"] == 2 and mesh.shape["dp"] == 2 and cols % 2 == 0
        fits = fits and units % 128 == 0 and sentences % (32 * SUBS) == 0 and steps % (2 * CHUNK) == 0
        return (fused if fits else shards)(tokens, w_input, w_recur, bias)

    return jax.shard_map(body, mesh=mesh, in_specs=in_specs, out_specs=out_specs, check_vma=False)
```
